32 devices in a mesh: dp: 2 (over x), expert: 8 (over z, y), tensor: 2 (over core).
Axes of the slice: x: 2, y: 2, z: 4, core: 2. Of those that a mesh axis runs over, the one named last changes fastest.
Arguments:
- tokens: bfloat16 [2048, 2048], P(('dp', 'expert')), may hold values from -6 to 6
- norm_gain: float32 [2048], replicated, may hold values from 0.1 to 1.9
- router: bfloat16 [2048, 8], replicated, may hold values from -0.125 to 0.125
- expert_ids: int32 [2048, 4], P(('dp', 'expert')), may hold values from 0 to 7, all different within a row; in each aligned block of 128 rows (0 to 127, 128 to 255, ...) at most 80 rows name the same one
- modality: int32 [2048], P(('dp', 'expert')), may hold values from 0 to 1, as said below
- expert_gate: bfloat16 [8, 2048, 1408], P('expert', None, 'tensor'), may hold values from -0.125 to 0.125
- expert_up: bfloat16 [8, 2048, 1408], P('expert', None, 'tensor'), may hold values from -0.125 to 0.125
- expert_down: bfloat16 [8, 1408, 2048], P('expert', 'tensor'), may hold values from -0.15625 to 0.15625
- shared_gate: bfloat16 [2, 2048, 704], P(None, None, ('dp', 'tensor')), may hold values from -0.125 to 0.125
- shared_up: bfloat16 [2, 2048, 704], P(None, None, ('dp', 'tensor')), may hold values from -0.125 to 0.125
- shared_down: bfloat16 [2, 704, 2048], P(None, ('dp', 'tensor')), may hold values from -0.21875 to 0.21875
Outputs:
- mixed: bfloat16 [2048, 2048], P(('dp', 'expert'), 'tensor')
The draws below stay inside these ranges and needn't reach their ends.
Inputs may be any that keep to these rules, and one draw needn't show every extreme that they name: `expert_ids`: each token names 4 different experts; among the 128 tokens of one device (aligned blocks of rows) no expert is named by more than 80 tokens, and some expert reaches 80. `modality`: within each aligned block of 128 tokens the image patches form one run (taken cyclically) that covers from an eighth to seven eighths of the block.
All inputs are finite; a program needn't handle non-finite values.
Results may differ from the reference program's by a relative error of at most 0.0073.
Values may be sent and summed in bfloat16 or wider, within the bound.
A program may use at most 128 MiB of HBM per device.

```python
import math
import jax
import jax.numpy as jnp
import numpy as np
from jax import lax

D = 2048
FF = 1408
SH = 704
TOP = 4
TOK_DEV = 128
EXPERTS = 8
TOKENS = 2048
CAP = 80


def draw_modality(key, part):
    blocks = TOKENS // TOK_DEV
    share_key, start_key = jax.random.split(jax.random.fold_in(key, 11))
    counts = jax.random.randint(share_key, (blocks, 1), TOK_DEV // 8, TOK_DEV - TOK_DEV // 8 + 1)
    starts = jax.random.randint(start_key, (blocks, 1), 0, TOK_DEV)
    position = jnp.arange(TOK_DEV, dtype=jnp.int32)[None, :]
    image_flags = ((position - starts) % TOK_DEV < counts).astype(jnp.int32)
    return image_flags.reshape(-1)


def steps_of(stream_key, shape, pieces, smallest, high):
    loudness, own = 1.0, jax.random.fold_in(stream_key, 6)
    for dim, blocks in pieces:
        draws = jnp.exp(jax.random.uniform(jax.random.fold_in(own, dim), (blocks,), jnp.float32, smallest / len(pieces), high / len(pieces)))
        loudness = loudness * jnp.repeat(draws, shape[dim] // blocks).reshape([-1 if axis == dim else 1 for axis in range(len(shape))])
    return loudness


def deal_out(rng, own, number, rows, amount, top, bound, slope):
    ranking = jax.random.permutation(rng, amount)
    heavy_load, usual = portions_of(amount, rows * top, bound, slope, True), portions_of(amount, rows * top, bound, slope, False)
    places = jnp.arange(amount)

    def named(tallies, rotation):
        used = int((tallies > 0).sum())
        fixed = max(1, used // 4)
        passed = fixed + (places - fixed + rotation * (used - fixed)) % max(1, amount - fixed)
        return jnp.zeros((amount,), jnp.int32).at[ranking[jnp.where(places < fixed, places, passed)]].set(jnp.asarray(tallies, jnp.int32))

    tallies = jnp.where(number % 4 == 0, named(heavy_load, number // 4), named(usual, number - number // 4 - 1))
    mixed = jax.random.permutation(jax.random.fold_in(own, 3), amount)
    giver, sink = mixed[0:amount // 2 * 2:2], mixed[1:amount // 2 * 2:2]
    margin = jnp.minimum(tallies[giver] - 1, bound - tallies[sink]) // 2
    margin = jnp.where((giver == ranking[0]) | (sink == ranking[0]) | (tallies[sink] == 0), 0, jnp.maximum(margin, 0))
    passed = jax.random.randint(jax.random.fold_in(own, 4), (amount // 2,), 0, 1 << 20) % (margin + 1)
    tallies = tallies.at[giver].add(-passed).at[sink].add(passed)
    labels = jnp.searchsorted(jnp.cumsum(tallies), jnp.arange(rows * top), side="right").astype(jnp.int32)
    listing = labels.reshape(top, rows).T
    listing = listing[jax.random.permutation(jax.random.fold_in(own, 1), rows)]
    rotation = jax.random.randint(jax.random.fold_in(own, 2), (rows, 1), 0, top)
    return jnp.take_along_axis(listing, (jnp.arange(top)[None, :] + rotation) % top, axis=1)


def portions_of(amount, total, reach, skew, full):
    weights = [(1 << 20) // math.isqrt(rank ** skew) + 1 for rank in range(1, amount + 1)]
    largest = reach if full else min(reach, max(-(-total // amount), total * weights[0] // sum(weights)))
    least = 1 if total - largest >= amount - 1 else 0
    given, spare = [largest] + [least] * (amount - 1), total - largest - least * (amount - 1)
    while spare > 0:
        free = [i for i in range(1, amount) if given[i] < largest] or [i for i in range(1, amount) if given[i] < reach]
        whole, left = sum([weights[i] for i in free]), spare
        for i in free:
            addition = min(reach - given[i], max(1, left * weights[i] // whole), spare)
            given[i] = given[i] + addition
            spare = spare - addition
    return np.array(given)


def bell_draw(rng, dims, scale, limit, pieces=(), held_as=jnp.bfloat16):
    array = scale * jax.random.normal(rng, dims, jnp.float32)
    if pieces:
        array = array * steps_of(rng, dims, pieces, -0.22, 0.18)
    return jnp.clip(array, -limit, limit).astype(held_as)


def setup_inputs(seed: int = 0) -> dict:
    key_list = jax.random.split(jax.random.key(seed), 12)
    tokens = bell_draw(key_list[0], (TOKENS, D), 1.0, 6.0, ((0, 16),))
    norm_gain = jnp.clip(1.0 + 0.18 * jax.random.normal(key_list[1], (D,), jnp.float32), 0.1, 1.9)
    router = bell_draw(key_list[2], (D, EXPERTS), D ** -0.5, 0.125)
    expert_ids_keys = jax.random.split(jax.random.fold_in(key_list[3], 1), TOKENS // TOK_DEV)
    expert_ids_turns = jax.random.permutation(jax.random.fold_in(key_list[3], 3), TOKENS // TOK_DEV)
    expert_ids = jax.vmap(lambda own, number: deal_out(jax.random.fold_in(key_list[3], 2), own, number, TOK_DEV, EXPERTS, TOP, CAP, 1))(expert_ids_keys, expert_ids_turns).reshape((TOKENS, TOP))
    modality = draw_modality(jax.random.fold_in(key_list[11], 71), 0)
    expert_gate = bell_draw(key_list[5], (EXPERTS, D, FF), D ** -0.5, 0.125, ((0, 8), (2, 2)))
    expert_up = bell_draw(key_list[6], (EXPERTS, D, FF), D ** -0.5, 0.125, ((0, 8), (2, 2)))
    expert_down = bell_draw(key_list[7], (EXPERTS, FF, D), FF ** -0.5, 0.15625, ((0, 8), (1, 2)))
    shared_gate = bell_draw(key_list[8], (2, D, SH), D ** -0.5, 0.125, ((2, 4),))
    shared_up = bell_draw(key_list[9], (2, D, SH), D ** -0.5, 0.125, ((2, 4),))
    shared_down = bell_draw(key_list[10], (2, SH, D), SH ** -0.5, 0.21875, ((1, 4),))
    return {"tokens": tokens, "norm_gain": norm_gain, "router": router, "expert_ids": expert_ids, "modality": modality, "expert_gate": expert_gate, "expert_up": expert_up, "expert_down": expert_down, "shared_gate": shared_gate, "shared_up": shared_up, "shared_down": shared_down}


epsilon = 1e-06

def rms_normed(tokens, norm_gain):
    values = tokens.astype(jnp.float32)
    inv_scale = lax.rsqrt(lax.optimization_barrier(jnp.mean(values * values, axis=-1, keepdims=True)) + epsilon)
    return (values * inv_scale * norm_gain).astype(jnp.bfloat16)

def route_weights(normed, router, expert_ids):
    logits = jnp.dot(normed, router, preferred_element_type=jnp.float32)
    chosen = jnp.take_along_axis(logits, expert_ids, axis=1)
    scores = jax.nn.sigmoid(chosen)
    return scores / lax.optimization_barrier(jnp.sum(scores, axis=1, keepdims=True))

def capacity_slots(expert_ids, expert_count, block_rows):
    row_count, top_count = expert_ids.shape
    onehot = (expert_ids[:, :, None] == jnp.arange(expert_count, dtype=jnp.int32)[None, None, :]).astype(jnp.int32)
    grouped = onehot.reshape(row_count // block_rows, block_rows * top_count, expert_count)
    running = (jnp.cumsum(grouped, axis=1, dtype=jnp.int32) - 1).reshape(row_count, top_count, expert_count)
    return lax.optimization_barrier(jnp.sum(running * onehot, axis=-1, dtype=jnp.int32)).astype(jnp.int32)

def reference(tokens, norm_gain, router, expert_ids, modality, expert_gate, expert_up, expert_down, shared_gate, shared_up, shared_down):
    normed = rms_normed(tokens, norm_gain)
    weights = route_weights(normed, router, expert_ids)
    slot_rank = capacity_slots(expert_ids, EXPERTS, TOK_DEV)
    sources = TOKENS // TOK_DEV
    token_index = jnp.broadcast_to(jnp.arange(TOKENS, dtype=jnp.int32)[:, None], (TOKENS, TOP)).astype(jnp.int32)
    source_block = (token_index // TOK_DEV).astype(jnp.int32)
    slot_table = jnp.full((EXPERTS, sources, CAP), TOKENS, jnp.int32)
    slot_table = slot_table.at[expert_ids, source_block, slot_rank].set(token_index)
    weight_table = jnp.zeros((EXPERTS, sources, CAP), jnp.float32)
    weight_table = weight_table.at[expert_ids, source_block, slot_rank].set(weights)
    padded = jnp.concatenate([normed, jnp.zeros((1, D), jnp.bfloat16)], axis=0)

    def one_expert(routed, operands):
        rows_index, slot_weight, gate_weight, up_weight, down_weight = operands
        flat_index = rows_index.reshape(-1)
        gathered = padded[flat_index]
        gate_value = jnp.dot(gathered, gate_weight, preferred_element_type=jnp.float32)
        up_value = jnp.dot(gathered, up_weight, preferred_element_type=jnp.float32)
        hidden = (jax.nn.silu(gate_value) * up_value).astype(jnp.bfloat16)
        result = jnp.dot(hidden, down_weight, preferred_element_type=jnp.float32)
        result = result * slot_weight.reshape(-1)[:, None]
        return (routed.at[flat_index].add(result), None)
    start = jnp.zeros((TOKENS + 1, D), jnp.float32)
    routed, unused = lax.scan(one_expert, start, (slot_table, weight_table, expert_gate, expert_up, expert_down))
    routed = routed[:TOKENS]

    def shared_out(modal_index):
        gate_value = jnp.dot(normed, shared_gate[modal_index], preferred_element_type=jnp.float32)
        up_value = jnp.dot(normed, shared_up[modal_index], preferred_element_type=jnp.float32)
        hidden = (jax.nn.silu(gate_value) * up_value).astype(jnp.bfloat16)
        return jnp.dot(hidden, shared_down[modal_index], preferred_element_type=jnp.float32)
    is_image = (modality == 1)[:, None]
    shared = jnp.where(is_image, shared_out(0), shared_out(1))
    return (shared + routed).astype(jnp.bfloat16)
```

```python
import jax
import jax.numpy as jnp
from jax import lax
from jax.experimental import pallas as pl
from jax.experimental.pallas import tpu as pltpu
from jax.sharding import PartitionSpec as P
import functools

epsilon = 1e-06


def rms_normed(tokens, norm_gain):
    values = tokens.astype(jnp.float32)
    inv_scale = lax.rsqrt(jnp.mean(values * values, axis=-1, keepdims=True) + epsilon)
    return (values * inv_scale * norm_gain).astype(jnp.bfloat16)


def route_weights(normed, router, expert_ids):
    logits = jnp.dot(normed, router, preferred_element_type=jnp.float32)
    chosen = jnp.take_along_axis(logits, expert_ids, axis=1)
    scores = jax.nn.sigmoid(chosen)
    return scores / jnp.sum(scores, axis=1, keepdims=True)


def capacity_slots(expert_ids, expert_count, block_rows):
    row_count, top_count = expert_ids.shape
    onehot = (
        expert_ids[:, :, None] == jnp.arange(expert_count, dtype=jnp.int32)[None, None, :]
    ).astype(jnp.int32)
    grouped = onehot.reshape(row_count // block_rows, block_rows * top_count, expert_count)
    running = (jnp.cumsum(grouped, axis=1, dtype=jnp.int32) - 1).reshape(
        row_count, top_count, expert_count
    )
    return jnp.sum(running * onehot, axis=-1, dtype=jnp.int32)


def gathered_per_device(
    tokens,
    norm_gain,
    router,
    expert_ids,
    modality,
    expert_gate,
    expert_up,
    expert_down,
    shared_gate,
    shared_up,
    shared_down,
):
    normed = rms_normed(tokens, norm_gain)
    weights = route_weights(normed, router, expert_ids)
    tok_rows, model_width = normed.shape
    top_count = expert_ids.shape[1]
    groups = lax.axis_size("expert")
    pair_count = lax.axis_size("tensor")
    dp_count = lax.axis_size("dp")
    half_width = model_width // pair_count
    expert_count = groups * expert_gate.shape[0]
    capacity = pair_count * (
        (5 * tok_rows * top_count + 4 * expert_count * pair_count - 1)
        // (4 * expert_count * pair_count)
    )
    slot_rank = capacity_slots(expert_ids, expert_count, tok_rows)
    target = expert_ids * capacity + slot_rank
    positions = jnp.arange(expert_count * capacity, dtype=jnp.int32)
    placing = jnp.any(positions[:, None, None] == target[None, :, :], axis=2).astype(jnp.bfloat16)
    outgoing = jnp.dot(placing, normed, preferred_element_type=jnp.float32).astype(jnp.bfloat16)
    outgoing = outgoing.reshape(groups, capacity, model_width)
    received = lax.all_to_all(outgoing, "expert", split_axis=0, concat_axis=0, tiled=True)
    flat_rows = received.reshape(-1, model_width)
    gate_value = jnp.dot(flat_rows, expert_gate[0], preferred_element_type=jnp.float32)
    up_value = jnp.dot(flat_rows, expert_up[0], preferred_element_type=jnp.float32)
    hidden = (jax.nn.silu(gate_value) * up_value).astype(jnp.bfloat16)
    result = jnp.dot(hidden, expert_down[0], preferred_element_type=jnp.float32)
    partials = result.reshape(received.shape[0], received.shape[1], model_width)
    reduced = lax.psum_scatter(partials, "tensor", scatter_dimension=2, tiled=True)
    returned = lax.all_to_all(reduced, "expert", split_axis=0, concat_axis=0, tiled=True)
    picked = returned.reshape(-1, returned.shape[2])[target]
    routed = jnp.sum(weights[:, :, None] * picked, axis=1)
    everyone, kind_flags = (
        lax.all_gather(normed, "dp", axis=0, tiled=True),
        lax.all_gather(modality, "dp", axis=0, tiled=True),
    )
    image_flag = kind_flags.astype(jnp.float32)[:, None]

    def shared_hidden(modal_index, keep):
        gate_value = jnp.dot(everyone, shared_gate[modal_index], preferred_element_type=jnp.float32)
        up_value = jnp.dot(everyone, shared_up[modal_index], preferred_element_type=jnp.float32)
        return (jax.nn.silu(gate_value) * up_value * keep).astype(jnp.bfloat16)

    joined = jnp.concatenate(
        [shared_hidden(0, image_flag), shared_hidden(1, 1.0 - image_flag)], axis=1
    )
    down_blocks = shared_down.reshape(-1, pair_count, half_width)
    split_rows = joined.reshape(dp_count, tok_rows, joined.shape[1])
    shared_term = jnp.einsum(
        "pks,std->ptkd", split_rows, down_blocks, preferred_element_type=jnp.float32
    )
    shared_sum = lax.psum_scatter(
        shared_term.reshape(-1, half_width), ("dp", "tensor"), scatter_dimension=0, tiled=True
    )
    total = shared_sum + routed
    return total.astype(jnp.bfloat16)


MESH = pl.DeviceIdType.MESH


def fused_kernel(
    n,
    tokens_ref,
    gain_ref,
    router_ref,
    ids_ref,
    kind_ref,
    wg_hbm,
    wu_hbm,
    wd_hbm,
    sg_hbm,
    su_hbm,
    sd_hbm,
    out_ref,
    x_buf,
    wt_buf,
    wg,
    wu,
    wd,
    sg,
    su,
    sd,
    hid,
    shid,
    part,
    sib_out,
    sib_in,
    rs_out,
    rs_in,
    dp_out,
    dp_in,
    w_sem,
    ag_send,
    ag_recv,
    sx_send,
    sx_recv,
    wt_send,
    wt_recv,
    dp_send,
    dp_recv,
    sr_send,
    sr_recv,
    rs_send,
    rs_recv,
):
    dp = lax.axis_index("dp")
    me = lax.axis_index("expert")
    core = lax.axis_index("tensor")
    other = 1 - core
    far = n // 2
    rows, width = tokens_ref.shape
    half = width // 2
    cut = rows // 2
    expert_count = router_ref.shape[1]
    ring = (me % 2) * (n - 1 - me // 2) + (1 - me % 2) * (me // 2)

    def at_ring(offset):
        spot = (ring + offset + n) % n
        late = spot // far
        return late * (2 * (n - 1 - spot) + 1) + (1 - late) * (2 * spot)

    def peer(offset):
        return (dp, at_ring(offset), core)

    sibling = (dp, me, other)
    across = (1 - dp, me, core)

    def left_slot(d):
        return n - 1 if d == far else 2 * d - 1

    def right_slot(d):
        return n - 1 if d == far else 2 * d

    def piece(k):
        return pl.ds(k * cut, cut)

    loads = [
        pltpu.make_async_copy(wg_hbm.at[0], wg, w_sem.at[0]),
        pltpu.make_async_copy(wu_hbm.at[0], wu, w_sem.at[1]),
        pltpu.make_async_copy(wd_hbm.at[0, :, pl.ds(0, half)], wd.at[0], w_sem.at[2]),
        pltpu.make_async_copy(wd_hbm.at[0, :, pl.ds(half, half)], wd.at[1], w_sem.at[3]),
        pltpu.make_async_copy(sg_hbm, sg, w_sem.at[4]),
        pltpu.make_async_copy(su_hbm, su, w_sem.at[5]),
        pltpu.make_async_copy(sd_hbm.at[:, :, pl.ds(0, half)], sd.at[0], w_sem.at[6]),
        pltpu.make_async_copy(sd_hbm.at[:, :, pl.ds(half, half)], sd.at[1], w_sem.at[7]),
    ]
    for load in loads:
        load.start()

    barrier = pltpu.get_barrier_semaphore()
    greeted = [peer(d) for d in range(1, n)] + [sibling, across]
    for device in greeted:
        pl.semaphore_signal(barrier, inc=1, device_id=device, device_id_type=MESH)

    values = tokens_ref[...].astype(jnp.float32)
    inv_scale = lax.rsqrt(jnp.mean(values * values, axis=-1, keepdims=True) + epsilon)
    normed = (values * inv_scale * gain_ref[...]).astype(jnp.bfloat16)
    x_buf[0, 0] = normed[:, :half]
    x_buf[0, 1] = normed[:, half:]
    logits = jnp.dot(normed, router_ref[...], preferred_element_type=jnp.float32)
    lanes = lax.broadcasted_iota(jnp.int32, (rows, expert_count), 1)
    chosen = lanes < 0
    for k in range(ids_ref.shape[1]):
        chosen = chosen | (ids_ref[:, k : k + 1] == lanes)
    scores = jnp.where(chosen, jax.nn.sigmoid(logits), 0.0)
    weights = scores / jnp.sum(scores, axis=1, keepdims=True)
    padded = jnp.concatenate(
        [weights, jnp.zeros((rows, rows - expert_count), jnp.float32)], axis=1
    )
    wt_buf[0, 0:expert_count] = padded.T[0:expert_count]
    flags = kind_ref[...].astype(jnp.float32)
    wt_buf[0, expert_count : expert_count + 8] = jnp.broadcast_to(flags, (8, rows))

    pl.semaphore_wait(barrier, len(greeted))

    started = []

    def remote(src, dst, send, recv, device):
        return pltpu.make_async_remote_copy(
            src_ref=src,
            dst_ref=dst,
            send_sem=send,
            recv_sem=recv,
            device_id=device,
            device_id_type=MESH,
        )

    def send(*copy):
        made = remote(*copy)
        made.start()
        started.append(made)

    def gather_copy(way, d, k):
        slot_of = (left_slot, right_slot)[way]
        src = x_buf.at[0 if d == 1 else slot_of(d - 1), core, piece(k)]
        dst = x_buf.at[slot_of(d), core, piece(k)]
        return (
            src,
            dst,
            ag_send.at[way, d - 1, k],
            ag_recv.at[way, d - 1, k],
            peer(1 if way == 0 else -1),
        )

    def swap_copy(way, d, k, mine):
        slot = (left_slot, right_slot)[way](d)
        block = x_buf.at[slot, core if mine else other, piece(k)]
        return (block, block, sx_send.at[way, d - 1, k], sx_recv.at[way, d - 1, k], sibling)

    def weight_copy(d):
        slot = 2 * d - 1 if d < far else (n - 1 if d == far else 2 * (n - d))
        return (wt_buf.at[0], wt_buf.at[slot], wt_send.at[slot], wt_recv.at[slot], peer(d))

    for k in range(2):
        for way in range(2):
            send(*gather_copy(way, 1, k))
        if k == 0:
            send(wt_buf.at[0], wt_buf.at[n], wt_send.at[n], wt_recv.at[n], across)
            send(x_buf.at[0, core], x_buf.at[n, core], dp_send.at[0], dp_recv.at[0], across)
            for d in range(1, n):
                send(*weight_copy(d))

    def forward(d, k):
        for way in range(2):
            if d == far and way != k:
                continue
            remote(*gather_copy(way, d, k)).wait_recv()
            if d + 1 < far or (d + 1 == far and way == k):
                send(*gather_copy(way, d + 1, k))
            send(*swap_copy(way, d, k, True))

    def swapped(d):
        for k in range(2):
            for way in range(2):
                if d == far and way != k:
                    continue
                remote(*swap_copy(way, d, k, False)).wait_recv()

    def column(row):
        return jnp.broadcast_to(row, (rows, rows)).T[:, 0:1]

    def rows_of(slots, part_index):
        blocks = [x_buf[slot, part_index] for slot in slots]
        return blocks[0] if len(blocks) == 1 else jnp.concatenate(blocks, axis=0)

    def double_dot(slots, low, high):
        return jnp.dot(
            rows_of(slots, 0), low, preferred_element_type=jnp.float32
        ) + jnp.dot(rows_of(slots, 1), high, preferred_element_type=jnp.float32)

    def expert_up_part(slots):
        for slot in slots:
            if slot != 0:
                block = wt_buf.at[slot]
                remote(
                    block, block, wt_send.at[slot], wt_recv.at[slot], sibling
                ).wait_recv()
        gate_value = double_dot(slots, wg[0:half], wg[half:width])
        up_value = double_dot(slots, wu[0:half], wu[half:width])
        scale = [column(wt_buf[slot, pl.ds(me, 1), :]) for slot in slots]
        scale = scale[0] if len(scale) == 1 else jnp.concatenate(scale, axis=0)
        hidden = (gate_value / (1.0 + jnp.exp(-gate_value))) * up_value * scale
        hid[0 : len(slots) * rows] = hidden.astype(jnp.bfloat16)

    def give(slot):
        return (
            sib_out.at[slot],
            sib_in.at[slot],
            sr_send.at[slot],
            sr_recv.at[slot],
            sibling,
        )

    def expert_down_part(slots):
        hidden = hid[0 : len(slots) * rows]
        theirs = jnp.dot(hidden, wd[other], preferred_element_type=jnp.float32)
        for i, slot in enumerate(slots):
            block = theirs[i * rows : (i + 1) * rows]
            if slot == 0:
                part[n + 1] = block
            else:
                sib_out[slot] = block.astype(jnp.bfloat16)
                send(*give(slot))
        mine = jnp.dot(hidden, wd[core], preferred_element_type=jnp.float32)
        for i, slot in enumerate(slots):
            part[slot] = mine[i * rows : (i + 1) * rows]

    def shared_part():
        slots = (0, n)
        flag = jnp.concatenate(
            [column(wt_buf[slot, expert_count : expert_count + 1, :]) for slot in slots], axis=0
        )
        mine = theirs = None
        for m, keep in enumerate((flag, 1.0 - flag)):
            gate_value = double_dot(slots, sg[m, 0:half], sg[m, half:width])
            up_value = double_dot(slots, su[m, 0:half], su[m, half:width])
            hidden = (gate_value / (1.0 + jnp.exp(-gate_value))) * up_value * keep
            shid[m] = hidden.astype(jnp.bfloat16)
        def down(which):
            return jnp.dot(
                shid[0], sd[which, 0], preferred_element_type=jnp.float32
            ) + jnp.dot(shid[1], sd[which, 1], preferred_element_type=jnp.float32)
        theirs = down(other)
        sib_out[0] = (theirs[:rows] + part[n + 1]).astype(jnp.bfloat16)
        sib_out[n] = theirs[rows:].astype(jnp.bfloat16)
        send(*give(n))
        send(*give(0))
        mine = down(core)
        part[0] = part[0] + mine[:rows]
        part[n] = mine[rows:]

    def shared_return():
        remote(*give(n)).wait_recv()
        dp_out[...] = (part[n] + sib_in[n].astype(jnp.float32)).astype(jnp.bfloat16)
        send(dp_out, dp_in, dp_send.at[1], dp_recv.at[1], across)

    def reduce_copy(way, d, k):
        return (
            rs_out.at[way, d - 1, piece(k)],
            rs_in.at[way, d - 1, piece(k)],
            rs_send.at[way, d - 1, k],
            rs_recv.at[way, d - 1, k],
            peer(1 if way == 0 else -1),
        )

    def reduce_step(way, d, k):
        slot = (right_slot, left_slot)[way](d)
        total = part[slot, piece(k)] + sib_in[slot, piece(k)].astype(jnp.float32)
        if d + 1 < far or (d + 1 == far and way == k):
            remote(*reduce_copy(way, d + 1, k)).wait_recv()
            total = total + rs_in[way, d, piece(k)].astype(jnp.float32)
        rs_out[way, d - 1, piece(k)] = total.astype(jnp.bfloat16)
        send(*reduce_copy(way, d, k))

    for load in loads[:4]:
        load.wait()
    expert_up_part((0,))
    forward(1, 0)
    expert_down_part((0,))
    for load in loads[4:]:
        load.wait()
    forward(1, 1)
    swapped(1)
    for d in range(1, far):
        slots = (left_slot(d), right_slot(d))
        expert_up_part(slots)
        forward(d + 1, 0)
        if d == 1:
            remote(x_buf.at[0, core], x_buf.at[n, core], dp_send.at[0], dp_recv.at[0], across).wait_recv()
            block = x_buf.at[n, core]
            send(block, block, sx_send.at[0, far, 0], sx_recv.at[0, far, 0], sibling)
        expert_down_part(slots)
        forward(d + 1, 1)
        if d == 1:
            block = x_buf.at[n, other]
            remote(block, block, sx_send.at[0, far, 0], sx_recv.at[0, far, 0], sibling).wait_recv()
            block = wt_buf.at[n]
            remote(block, block, wt_send.at[n], wt_recv.at[n], across).wait_recv()
            shared_part()
        swapped(d + 1)
        if d == 2:
            shared_return()
    expert_up_part((n - 1,))
    expert_down_part((n - 1,))
    for slot in (left_slot(far - 1), right_slot(far - 1)):
        remote(*give(slot)).wait_recv()
    reduce_step(0, far - 1, 1)
    reduce_step(1, far - 1, 0)
    remote(*give(n - 1)).wait_recv()
    reduce_step(0, far, 0)
    reduce_step(1, far, 1)
    for d in range(far - 2, 0, -1):
        for slot in (left_slot(d), right_slot(d)):
            remote(*give(slot)).wait_recv()
    remote(*give(0)).wait_recv()
    reduce_step(0, far - 1, 0)
    reduce_step(1, far - 1, 1)
    for d in range(far - 2, 0, -1):
        reduce_step(0, d, 1)
        reduce_step(1, d, 0)
        reduce_step(0, d, 0)
        reduce_step(1, d, 1)
    remote(dp_out, dp_in, dp_send.at[1], dp_recv.at[1], across).wait_recv()
    base = part[0] + sib_in[0].astype(jnp.float32) + dp_in[...].astype(jnp.float32)
    part[0] = base
    for k in (1, 0):
        for way in (0, 1):
            if far == 1 and way != k:
                continue
            remote(*reduce_copy(way, 1, k)).wait_recv()
    for k in range(2):
        total = part[0, piece(k)]
        for way in range(2):
            total = total + rs_in[way, 0, piece(k)].astype(jnp.float32)
        out_ref[piece(k)] = total.astype(out_ref.dtype)
    for made in started:
        made.wait_send()


def fused_per_device(
    tokens,
    norm_gain,
    router,
    expert_ids,
    modality,
    expert_gate,
    expert_up,
    expert_down,
    shared_gate,
    shared_up,
    shared_down,
):
    n = lax.axis_size("expert")
    rows, width = tokens.shape
    half = width // 2
    far = n // 2
    hidden = expert_gate.shape[2]
    shared = shared_gate.shape[2]
    held = router.shape[1] + 8
    bf16, f32 = jnp.bfloat16, jnp.float32
    dma = pltpu.SemaphoreType.DMA
    scratch = [
        pltpu.VMEM((n + 1, 2, rows, half), bf16),
        pltpu.VMEM((n + 1, held, rows), f32),
        pltpu.VMEM((width, hidden), bf16),
        pltpu.VMEM((width, hidden), bf16),
        pltpu.VMEM((2, hidden, half), bf16),
        pltpu.VMEM((2, width, shared), bf16),
        pltpu.VMEM((2, width, shared), bf16),
        pltpu.VMEM((2, 2, shared, half), bf16),
        pltpu.VMEM((2 * rows, hidden), bf16),
        pltpu.VMEM((2, 2 * rows, shared), bf16),
        pltpu.VMEM((n + 2, rows, half), f32),
        pltpu.VMEM((n + 1, rows, half), bf16),
        pltpu.VMEM((n + 1, rows, half), bf16),
        pltpu.VMEM((2, far, rows, half), bf16),
        pltpu.VMEM((2, far, rows, half), bf16),
        pltpu.VMEM((rows, half), bf16),
        pltpu.VMEM((rows, half), bf16),
        dma((8,)),
        dma((2, far, 2)),
        dma((2, far, 2)),
        dma((2, far + 1, 2)),
        dma((2, far + 1, 2)),
        dma((n + 1,)),
        dma((n + 1,)),
        dma((2,)),
        dma((2,)),
        dma((n + 1,)),
        dma((n + 1,)),
        dma((2, far, 2)),
        dma((2, far, 2)),
    ]
    vmem = pl.BlockSpec(memory_space=pltpu.VMEM)
    anywhere = pl.BlockSpec(memory_space=pl.ANY)
    return pl.pallas_call(
        functools.partial(fused_kernel, n),
        out_shape=jax.ShapeDtypeStruct((rows, half), bf16),
        in_specs=[vmem] * 5 + [anywhere] * 6,
        out_specs=vmem,
        scratch_shapes=scratch,
        compiler_params=pltpu.CompilerParams(
            collective_id=0, has_side_effects=True, vmem_limit_bytes=60 * 1024 * 1024
        ),
    )(
        tokens,
        norm_gain.reshape(1, -1),
        router,
        expert_ids,
        modality.reshape(1, -1),
        expert_gate,
        expert_up,
        expert_down,
        shared_gate,
        shared_up,
        shared_down,
    )


def per_device(*arrays):
    tokens, expert_gate, router = arrays[0], arrays[5], arrays[2]
    n = lax.axis_size("expert")
    block_bytes = tokens.shape[0] * tokens.shape[1] * 2
    weight_bytes = sum(2 * array.size for array in arrays[5:])
    fits = 9 * n * block_bytes // 2 + weight_bytes < 40 * 1024 * 1024
    square = tokens.shape[0] == 128 and lax.axis_size("tensor") == 2 and lax.axis_size("dp") == 2
    if fits and square and n >= 6 and n % 2 == 0 and expert_gate.shape[0] == 1:
        return fused_per_device(*arrays)
    return gathered_per_device(*arrays)


def solution(mesh):
    in_specs = (
        P(("dp", "expert"), None),
        P(),
        P(),
        P(("dp", "expert"), None),
        P(("dp", "expert")),
        P("expert", None, "tensor"),
        P("expert", None, "tensor"),
        P("expert", "tensor", None),
        P(None, None, ("dp", "tensor")),
        P(None, None, ("dp", "tensor")),
        P(None, ("dp", "tensor"), None),
    )
    out_specs = P(("dp", "expert"), "tensor")
    return jax.shard_map(
        per_device, mesh=mesh, in_specs=in_specs, out_specs=out_specs, check_vma=False
    )
```

```python
import jax
import jax.numpy as jnp
from jax import lax
from jax.experimental import pallas as pl
from jax.experimental.pallas import tpu as pltpu
from jax.sharding import PartitionSpec as P
import functools

epsilon = 1e-06


def rms_normed(tokens, norm_gain):
    values = tokens.astype(jnp.float32)
    inv_scale = lax.rsqrt(jnp.mean(values * values, axis=-1, keepdims=True) + epsilon)
    return (values * inv_scale * norm_gain).astype(jnp.bfloat16)


def route_weights(normed, router, expert_ids):
    logits = jnp.dot(normed, router, preferred_element_type=jnp.float32)
    chosen = jnp.take_along_axis(logits, expert_ids, axis=1)
    scores = jax.nn.sigmoid(chosen)
    return scores / jnp.sum(scores, axis=1, keepdims=True)


def capacity_slots(expert_ids, expert_count, block_rows):
    row_count, top_count = expert_ids.shape
    onehot = (
        expert_ids[:, :, None] == jnp.arange(expert_count, dtype=jnp.int32)[None, None, :]
    ).astype(jnp.int32)
    grouped = onehot.reshape(row_count // block_rows, block_rows * top_count, expert_count)
    running = (jnp.cumsum(grouped, axis=1, dtype=jnp.int32) - 1).reshape(
        row_count, top_count, expert_count
    )
    return jnp.sum(running * onehot, axis=-1, dtype=jnp.int32)


def gathered_per_device(
    tokens,
    norm_gain,
    router,
    expert_ids,
    modality,
    expert_gate,
    expert_up,
    expert_down,
    shared_gate,
    shared_up,
    shared_down,
):
    normed = rms_normed(tokens, norm_gain)
    weights = route_weights(normed, router, expert_ids)
    tok_rows, model_width = normed.shape
    top_count = expert_ids.shape[1]
    groups = lax.axis_size("expert")
    pair_count = lax.axis_size("tensor")
    dp_count = lax.axis_size("dp")
    half_width = model_width // pair_count
    expert_count = groups * expert_gate.shape[0]
    capacity = pair_count * (
        (5 * tok_rows * top_count + 4 * expert_count * pair_count - 1)
        // (4 * expert_count * pair_count)
    )
    slot_rank = capacity_slots(expert_ids, expert_count, tok_rows)
    target = expert_ids * capacity + slot_rank
    positions = jnp.arange(expert_count * capacity, dtype=jnp.int32)
    placing = jnp.any(positions[:, None, None] == target[None, :, :], axis=2).astype(jnp.bfloat16)
    outgoing = jnp.dot(placing, normed, preferred_element_type=jnp.float32).astype(jnp.bfloat16)
    outgoing = outgoing.reshape(groups, capacity, model_width)
    received = lax.all_to_all(outgoing, "expert", split_axis=0, concat_axis=0, tiled=True)
    flat_rows = received.reshape(-1, model_width)
    gate_value = jnp.dot(flat_rows, expert_gate[0], preferred_element_type=jnp.float32)
    up_value = jnp.dot(flat_rows, expert_up[0], preferred_element_type=jnp.float32)
    hidden = (jax.nn.silu(gate_value) * up_value).astype(jnp.bfloat16)
    result = jnp.dot(hidden, expert_down[0], preferred_element_type=jnp.float32)
    partials = result.reshape(received.shape[0], received.shape[1], model_width)
    reduced = lax.psum_scatter(partials, "tensor", scatter_dimension=2, tiled=True)
    returned = lax.all_to_all(reduced, "expert", split_axis=0, concat_axis=0, tiled=True)
    picked = returned.reshape(-1, returned.shape[2])[target]
    routed = jnp.sum(weights[:, :, None] * picked, axis=1)
    everyone, kind_flags = (
        lax.all_gather(normed, "dp", axis=0, tiled=True),
        lax.all_gather(modality, "dp", axis=0, tiled=True),
    )
    image_flag = kind_flags.astype(jnp.float32)[:, None]

    def shared_hidden(modal_index, keep):
        gate_value = jnp.dot(everyone, shared_gate[modal_index], preferred_element_type=jnp.float32)
        up_value = jnp.dot(everyone, shared_up[modal_index], preferred_element_type=jnp.float32)
        return (jax.nn.silu(gate_value) * up_value * keep).astype(jnp.bfloat16)

    joined = jnp.concatenate(
        [shared_hidden(0, image_flag), shared_hidden(1, 1.0 - image_flag)], axis=1
    )
    down_blocks = shared_down.reshape(-1, pair_count, half_width)
    split_rows = joined.reshape(dp_count, tok_rows, joined.shape[1])
    shared_term = jnp.einsum(
        "pks,std->ptkd", split_rows, down_blocks, preferred_element_type=jnp.float32
    )
    shared_sum = lax.psum_scatter(
        shared_term.reshape(-1, half_width), ("dp", "tensor"), scatter_dimension=0, tiled=True
    )
    total = shared_sum + routed
    return total.astype(jnp.bfloat16)


def across_dot(left, right):
    return lax.dot_general(
        left, right, (((1,), (1,)), ((), ())), preferred_element_type=jnp.float32
    )


MESH = pl.DeviceIdType.MESH


def fused_kernel(
    n,
    tokens_ref,
    gain_ref,
    router_ref,
    ids_ref,
    kind_ref,
    wg_hbm,
    wu_hbm,
    wd_hbm,
    sg_hbm,
    su_hbm,
    sd_hbm,
    out_ref,
    x_buf,
    wt_buf,
    wg,
    wu,
    wd,
    sg,
    su,
    sd,
    hid,
    shid,
    part,
    sib_out,
    sib_in,
    rs_out,
    rs_in,
    dp_out,
    dp_in,
    w_sem,
    ag_send,
    ag_recv,
    sx_send,
    sx_recv,
    wt_send,
    wt_recv,
    dp_send,
    dp_recv,
    sr_send,
    sr_recv,
    rs_send,
    rs_recv,
):
    dp = lax.axis_index("dp")
    me = lax.axis_index("expert")
    core = lax.axis_index("tensor")
    other = 1 - core
    far = n // 2
    rows, width = tokens_ref.shape
    half = width // 2
    cut = rows // 2
    expert_count = router_ref.shape[0]
    ring = (me % 2) * (n - 1 - me // 2) + (1 - me % 2) * (me // 2)

    def at_ring(offset):
        spot = (ring + offset + n) % n
        late = spot // far
        return late * (2 * (n - 1 - spot) + 1) + (1 - late) * (2 * spot)

    def peer(offset):
        return (dp, at_ring(offset), core)

    sibling = (dp, me, other)
    across = (1 - dp, me, core)

    def left_slot(d):
        return n - 1 if d == far else 2 * d - 1

    def right_slot(d):
        return n - 1 if d == far else 2 * d

    def piece(k):
        return pl.ds(k * cut, cut)

    loads = [
        pltpu.make_async_copy(wg_hbm.at[0], wg, w_sem.at[0]),
        pltpu.make_async_copy(wu_hbm.at[0], wu, w_sem.at[1]),
        pltpu.make_async_copy(wd_hbm.at[0, :, pl.ds(0, half)], wd.at[0], w_sem.at[2]),
        pltpu.make_async_copy(wd_hbm.at[0, :, pl.ds(half, half)], wd.at[1], w_sem.at[3]),
        pltpu.make_async_copy(sg_hbm, sg, w_sem.at[4]),
        pltpu.make_async_copy(su_hbm, su, w_sem.at[5]),
        pltpu.make_async_copy(sd_hbm.at[:, :, pl.ds(0, half)], sd.at[0], w_sem.at[6]),
        pltpu.make_async_copy(sd_hbm.at[:, :, pl.ds(half, half)], sd.at[1], w_sem.at[7]),
    ]
    for load in loads:
        load.start()

    barrier = pltpu.get_barrier_semaphore()
    greeted = [peer(d) for d in range(1, n)] + [sibling, across]
    for device in greeted:
        pl.semaphore_signal(barrier, inc=1, device_id=device, device_id_type=MESH)

    values = tokens_ref[...].astype(jnp.float32)
    inv_scale = lax.rsqrt(jnp.mean(values * values, axis=-1, keepdims=True) + epsilon)
    normed = (values * inv_scale * gain_ref[...]).astype(jnp.bfloat16)
    x_buf[0, 0] = normed[:, :half]
    x_buf[0, 1] = normed[:, half:]
    logits = across_dot(router_ref[...], normed)
    named = lax.broadcasted_iota(jnp.int32, (expert_count, rows), 0)
    chosen = named < 0
    for k in range(ids_ref.shape[0]):
        chosen = chosen | (ids_ref[k : k + 1, :] == named)
    scores = jnp.where(chosen, jax.nn.sigmoid(logits), 0.0)
    wt_buf[0, 0:expert_count] = scores / jnp.sum(scores, axis=0, keepdims=True)
    flags = kind_ref[...].astype(jnp.float32)
    wt_buf[0, expert_count : expert_count + 8] = jnp.broadcast_to(flags, (8, rows))

    pl.semaphore_wait(barrier, len(greeted))

    started = []

    def remote(src, dst, send, recv, device):
        return pltpu.make_async_remote_copy(
            src_ref=src,
            dst_ref=dst,
            send_sem=send,
            recv_sem=recv,
            device_id=device,
            device_id_type=MESH,
        )

    def send(*copy):
        made = remote(*copy)
        made.start()
        started.append(made)

    def gather_copy(way, d, k):
        slot_of = (left_slot, right_slot)[way]
        src = x_buf.at[0 if d == 1 else slot_of(d - 1), core, piece(k)]
        dst = x_buf.at[slot_of(d), core, piece(k)]
        return (
            src,
            dst,
            ag_send.at[way, d - 1, k],
            ag_recv.at[way, d - 1, k],
            peer(1 if way == 0 else -1),
        )

    def swap_copy(way, d, k, mine):
        slot = (left_slot, right_slot)[way](d)
        block = x_buf.at[slot, core if mine else other, piece(k)]
        return (block, block, sx_send.at[way, d - 1, k], sx_recv.at[way, d - 1, k], sibling)

    def weight_copy(d):
        slot = 2 * d - 1 if d < far else (n - 1 if d == far else 2 * (n - d))
        return (wt_buf.at[0], wt_buf.at[slot], wt_send.at[slot], wt_recv.at[slot], peer(d))

    for turn in range(2):
        for way in range(2):
            send(*gather_copy(way, 1, (way + turn) % 2))
        if turn == 0:
            send(wt_buf.at[0], wt_buf.at[n], wt_send.at[n], wt_recv.at[n], across)
            send(x_buf.at[0, core], x_buf.at[n, core], dp_send.at[0], dp_recv.at[0], across)
            for d in range(1, n):
                send(*weight_copy(d))

    def forward(d, turn):
        for way in range(2):
            k = (way + turn) % 2
            remote(*gather_copy(way, d, k)).wait_recv()
            if d + 1 < far or (d + 1 == far and turn == 0):
                send(*gather_copy(way, d + 1, k))
            send(*swap_copy(way, d, k, True))

    def swapped(d, turn):
        for way in range(2):
            remote(*swap_copy(way, d, (way + turn) % 2, False)).wait_recv()

    def column(row):
        return jnp.broadcast_to(row, (rows, rows)).T[:, 0:1]

    def whole(*slots):
        return [(slot, 0, rows) for slot in slots]

    def joined(blocks):
        return blocks[0] if len(blocks) == 1 else jnp.concatenate(blocks, axis=0)

    def rows_of(pieces, part_index):
        return joined([x_buf[slot, part_index, lo : lo + size] for slot, lo, size in pieces])

    def double_dot(pieces, low, high):
        return across_dot(rows_of(pieces, 0), low) + across_dot(rows_of(pieces, 1), high)

    def weights_here(*slots):
        for slot in slots:
            block = wt_buf.at[slot]
            remote(block, block, wt_send.at[slot], wt_recv.at[slot], sibling).wait_recv()

    def expert_up_part(pieces):
        count = sum(size for slot, lo, size in pieces)
        gate_value = double_dot(pieces, wg[:, 0:half], wg[:, half:width])
        up_value = double_dot(pieces, wu[:, 0:half], wu[:, half:width])
        scale = joined(
            [column(wt_buf[slot, pl.ds(me, 1), :])[lo : lo + size] for slot, lo, size in pieces]
        )
        hidden = (gate_value / (1.0 + jnp.exp(-gate_value))) * up_value * scale
        hid[0:count] = hidden.astype(jnp.bfloat16)

    def give(slot, lo=0, size=rows):
        block = pl.ds(lo, size)
        return (
            sib_out.at[slot, block],
            sib_in.at[slot, block],
            sr_send.at[slot, lo // cut],
            sr_recv.at[slot, lo // cut],
            sibling,
        )

    def given(*pieces):
        for piece_given in pieces:
            remote(*give(*piece_given)).wait_recv()

    def expert_down_part(pieces):
        count = sum(size for slot, lo, size in pieces)
        hidden = hid[0:count]
        theirs = jnp.dot(hidden, wd[other], preferred_element_type=jnp.float32)
        first = 0
        for slot, lo, size in pieces:
            block = theirs[first : first + size]
            first += size
            if slot == 0:
                part[n + 1] = block
            else:
                sib_out[slot, lo : lo + size] = block.astype(jnp.bfloat16)
                send(*give(slot, lo, size))
        mine = jnp.dot(hidden, wd[core], preferred_element_type=jnp.float32)
        first = 0
        for slot, lo, size in pieces:
            part[slot, lo : lo + size] = mine[first : first + size]
            first += size

    def shared_part():
        slots = (0, n)
        pieces = whole(*slots)
        flag = jnp.concatenate(
            [column(wt_buf[slot, expert_count : expert_count + 1, :]) for slot in slots], axis=0
        )
        mine = theirs = None
        for m, keep in enumerate((flag, 1.0 - flag)):
            gate_value = double_dot(pieces, sg[m, :, 0:half], sg[m, :, half:width])
            up_value = double_dot(pieces, su[m, :, 0:half], su[m, :, half:width])
            hidden = (gate_value / (1.0 + jnp.exp(-gate_value))) * up_value * keep
            shid[m] = hidden.astype(jnp.bfloat16)
        def down(which):
            return jnp.dot(
                shid[0], sd[which, 0], preferred_element_type=jnp.float32
            ) + jnp.dot(shid[1], sd[which, 1], preferred_element_type=jnp.float32)
        theirs = down(other)
        sib_out[0] = (theirs[:rows] + part[n + 1]).astype(jnp.bfloat16)
        sib_out[n] = theirs[rows:].astype(jnp.bfloat16)
        send(*give(n))
        send(*give(0))
        mine = down(core)
        part[0] = part[0] + mine[:rows]
        part[n] = mine[rows:]

    def shared_return():
        given((n,))
        dp_out[...] = (part[n] + sib_in[n].astype(jnp.float32)).astype(jnp.bfloat16)
        send(dp_out, dp_in, dp_send.at[1], dp_recv.at[1], across)

    def reduce_copy(way, d, k):
        return (
            rs_out.at[way, d - 1, piece(k)],
            rs_in.at[way, d - 1, piece(k)],
            rs_send.at[way, d - 1, k],
            rs_recv.at[way, d - 1, k],
            peer(1 if way == 0 else -1),
        )

    def reduce_step(way, d, k):
        slot = (right_slot, left_slot)[way](d)
        total = part[slot, piece(k)] + sib_in[slot, piece(k)].astype(jnp.float32)
        if d + 1 < far or (d + 1 == far and way == k):
            remote(*reduce_copy(way, d + 1, k)).wait_recv()
            total = total + rs_in[way, d, piece(k)].astype(jnp.float32)
        rs_out[way, d - 1, piece(k)] = total.astype(jnp.bfloat16)
        send(*reduce_copy(way, d, k))

    for load in loads[:4]:
        load.wait()
    expert_up_part(whole(0))
    forward(1, 0)
    expert_down_part(whole(0))
    for load in loads[4:]:
        load.wait()
    forward(1, 1)
    for d in range(1, far - 1):
        pieces = whole(left_slot(d), right_slot(d))
        swapped(d, 0)
        swapped(d, 1)
        weights_here(left_slot(d), right_slot(d))
        expert_up_part(pieces)
        forward(d + 1, 0)
        if d == 1:
            remote(
                x_buf.at[0, core], x_buf.at[n, core], dp_send.at[0], dp_recv.at[0], across
            ).wait_recv()
            block = x_buf.at[n, core]
            send(block, block, sx_send.at[0, far, 0], sx_recv.at[0, far, 0], sibling)
        expert_down_part(pieces)
        forward(d + 1, 1)
        if d == 1:
            block = x_buf.at[n, other]
            remote(block, block, sx_send.at[0, far, 0], sx_recv.at[0, far, 0], sibling).wait_recv()
            weights_here(n)
            shared_part()
        if d == 2:
            shared_return()
    near = far - 1
    early = [(right_slot(near), cut, cut), (left_slot(near), 0, cut)]
    later = [(right_slot(near), 0, cut), (left_slot(near), cut, cut)]
    last = whole(n - 1)
    swapped(near, 0)
    weights_here(left_slot(near), right_slot(near))
    expert_up_part(early)
    expert_down_part(early)
    swapped(near, 1)
    expert_up_part(later)
    given(*early)
    reduce_step(0, near, 1)
    reduce_step(1, near, 0)
    expert_down_part(later)
    forward(far, 0)
    weights_here(n - 1)
    swapped(far, 0)
    expert_up_part(last)
    expert_down_part(last)
    given(*last)
    reduce_step(0, far, 0)
    reduce_step(1, far, 1)
    given(*later)
    for d in range(near - 1, 0, -1):
        given(*whole(left_slot(d), right_slot(d)))
    given(*whole(0))
    remote(dp_out, dp_in, dp_send.at[1], dp_recv.at[1], across).wait_recv()
    part[0] = part[0] + sib_in[0].astype(jnp.float32) + dp_in[...].astype(jnp.float32)
    reduce_step(0, near, 0)
    reduce_step(1, near, 1)
    for d in range(far - 2, 0, -1):
        reduce_step(0, d, 1)
        reduce_step(1, d, 0)
        reduce_step(0, d, 0)
        reduce_step(1, d, 1)
    for turn in range(2):
        for way in range(2):
            remote(*reduce_copy(way, 1, (way + 1 + turn) % 2)).wait_recv()
    for k in range(2):
        total = part[0, piece(k)]
        for way in range(2):
            total = total + rs_in[way, 0, piece(k)].astype(jnp.float32)
        out_ref[piece(k)] = total.astype(out_ref.dtype)
    for made in started:
        made.wait_send()


def fused_per_device(
    tokens,
    norm_gain,
    router,
    expert_ids,
    modality,
    expert_gate,
    expert_up,
    expert_down,
    shared_gate,
    shared_up,
    shared_down,
):
    n = lax.axis_size("expert")
    rows, width = tokens.shape
    half = width // 2
    far = n // 2
    hidden = expert_gate.shape[2]
    shared = shared_gate.shape[2]
    held = router.shape[1] + 8
    bf16, f32 = jnp.bfloat16, jnp.float32
    dma = pltpu.SemaphoreType.DMA
    scratch = [
        pltpu.VMEM((n + 1, 2, rows, half), bf16),
        pltpu.VMEM((n + 1, held, rows), f32),
        pltpu.VMEM((hidden, width), bf16),
        pltpu.VMEM((hidden, width), bf16),
        pltpu.VMEM((2, hidden, half), bf16),
        pltpu.VMEM((2, shared, width), bf16),
        pltpu.VMEM((2, shared, width), bf16),
        pltpu.VMEM((2, 2, shared, half), bf16),
        pltpu.VMEM((2 * rows, hidden), bf16),
        pltpu.VMEM((2, 2 * rows, shared), bf16),
        pltpu.VMEM((n + 2, rows, half), f32),
        pltpu.VMEM((n + 1, rows, half), bf16),
        pltpu.VMEM((n + 1, rows, half), bf16),
        pltpu.VMEM((2, far, rows, half), bf16),
        pltpu.VMEM((2, far, rows, half), bf16),
        pltpu.VMEM((rows, half), bf16),
        pltpu.VMEM((rows, half), bf16),
        dma((8,)),
        dma((2, far, 2)),
        dma((2, far, 2)),
        dma((2, far + 1, 2)),
        dma((2, far + 1, 2)),
        dma((n + 1,)),
        dma((n + 1,)),
        dma((2,)),
        dma((2,)),
        dma((n + 1, 2)),
        dma((n + 1, 2)),
        dma((2, far, 2)),
        dma((2, far, 2)),
    ]
    vmem = pl.BlockSpec(memory_space=pltpu.VMEM)
    anywhere = pl.BlockSpec(memory_space=pl.ANY)
    return pl.pallas_call(
        functools.partial(fused_kernel, n),
        out_shape=jax.ShapeDtypeStruct((rows, half), bf16),
        in_specs=[vmem] * 5 + [anywhere] * 6,
        out_specs=vmem,
        scratch_shapes=scratch,
        compiler_params=pltpu.CompilerParams(
            collective_id=0, has_side_effects=True, vmem_limit_bytes=60 * 1024 * 1024
        ),
    )(
        tokens,
        norm_gain.reshape(1, -1),
        router.T,
        expert_ids.T,
        modality.reshape(1, -1),
        jnp.swapaxes(expert_gate, 1, 2),
        jnp.swapaxes(expert_up, 1, 2),
        expert_down,
        jnp.swapaxes(shared_gate, 1, 2),
        jnp.swapaxes(shared_up, 1, 2),
        shared_down,
    )


def per_device(*arrays):
    tokens, expert_gate, router = arrays[0], arrays[5], arrays[2]
    n = lax.axis_size("expert")
    block_bytes = tokens.shape[0] * tokens.shape[1] * 2
    weight_bytes = sum(2 * array.size for array in arrays[5:])
    fits = 9 * n * block_bytes // 2 + weight_bytes < 40 * 1024 * 1024
    square = tokens.shape[0] == 128 and lax.axis_size("tensor") == 2 and lax.axis_size("dp") == 2
    if fits and square and n >= 6 and n % 2 == 0 and expert_gate.shape[0] == 1:
        return fused_per_device(*arrays)
    return gathered_per_device(*arrays)


def solution(mesh):
    in_specs = (
        P(("dp", "expert"), None),
        P(),
        P(),
        P(("dp", "expert"), None),
        P(("dp", "expert")),
        P("expert", None, "tensor"),
        P("expert", None, "tensor"),
        P("expert", "tensor", None),
        P(None, None, ("dp", "tensor")),
        P(None, None, ("dp", "tensor")),
        P(None, ("dp", "tensor"), None),
    )
    out_specs = P(("dp", "expert"), "tensor")
    return jax.shard_map(
        per_device, mesh=mesh, in_specs=in_specs, out_specs=out_specs, check_vma=False
    )
```
